8 devices in a mesh: dp: 1 (over z), tp: 8 (over y, x, core).
Axes of the slice: x: 2, y: 2, z: 1, core: 2. Of those that a mesh axis runs over, the one named last changes fastest.
Arguments:
- x_in: bfloat16 [4, 2048, 4608], P('dp', 'tp')
- positions: int32 [4, 2048], P('dp', 'tp')
- grad_out: bfloat16 [4, 2048, 4608], P('dp', 'tp')
- w_query: bfloat16 [4608, 32, 128], P(None, 'tp')
- w_key: bfloat16 [4608, 16, 128], P(None, 'tp')
- w_value: bfloat16 [4608, 16, 128], P(None, 'tp')
- w_out: bfloat16 [32, 128, 4608], P('tp')
- gain_pre: float32 [4608], replicated
- gain_post: float32 [4608], replicated
Outputs:
- output 1: bfloat16 [4, 2048, 4608], P('dp', 'tp')
- output 2: bfloat16 [4, 2048, 4608], P('dp', 'tp')
- output 3: float32 [4608, 32, 128], P('dp', 'tp')
- output 4: float32 [4608, 16, 128], P('dp', 'tp')
- output 5: float32 [4608, 16, 128], P('dp', 'tp')
- output 6: float32 [32, 128, 4608], P(('dp', 'tp'))
- output 7: float32 [4608], P('dp')
- output 8: float32 [4608], P('dp')
All inputs are finite; a program needn't handle non-finite values.
Results may differ from the reference program's by a relative error of at most 0.0177108.
Values are sent between devices in bfloat16 or wider.
A program may use at most 1 GiB of HBM per device.

```python
import functools
import jax
import jax.numpy as jnp
from jax import lax

BATCH_ROWS = 4
SEQ_LEN = 2048
MODEL_DIM = 4608
NUM_HEADS = 32
KV_HEADS = 16
HEAD_DIM = 128
WINDOW = 4096
QUERY_BLOCK = 128
SOFT_CAP = 50.0
NORM_EPS = 1e-6
ROPE_THETA = 10000.0


def draw_positions(pos_key, n_rows, seq_len):
    key_off, key_hit, key_jump = jax.random.split(pos_key, 3)
    offset = jax.random.randint(key_off, (n_rows, 1), 0, WINDOW)
    hit_draw = jax.random.randint(key_hit, (n_rows, seq_len), 0, max(seq_len // 8, 1))
    jump_size = jax.random.randint(key_jump, (n_rows, seq_len), 1, 2 * WINDOW)
    pos_steps = 1 + jnp.where(hit_draw == 0, jump_size, 0)
    return (offset + jnp.cumsum(pos_steps, axis=1) - pos_steps[:, :1]).astype(jnp.int32)


def setup_inputs(seed: int = 0, part: int = 0) -> dict:
    base_key = jax.random.key(seed)
    part_key = jax.random.fold_in(base_key, part)
    key_x, key_pos, key_dy = jax.random.split(part_key, 3)
    key_q, key_k, key_v, key_o, key_gp, key_gq = jax.random.split(base_key, 6)
    act_shape = (BATCH_ROWS, SEQ_LEN, MODEL_DIM)
    in_scale = MODEL_DIM ** -0.5
    out_scale = (NUM_HEADS * HEAD_DIM) ** -0.5
    x_in = jax.random.normal(key_x, act_shape, jnp.float32).astype(jnp.bfloat16)
    positions = draw_positions(key_pos, BATCH_ROWS, SEQ_LEN)
    grad_out = jax.random.normal(key_dy, act_shape, jnp.float32).astype(jnp.bfloat16)
    w_query = (jax.random.normal(key_q, (MODEL_DIM, NUM_HEADS, HEAD_DIM), jnp.float32) * in_scale).astype(jnp.bfloat16)
    w_key = (jax.random.normal(key_k, (MODEL_DIM, KV_HEADS, HEAD_DIM), jnp.float32) * in_scale).astype(jnp.bfloat16)
    w_value = (jax.random.normal(key_v, (MODEL_DIM, KV_HEADS, HEAD_DIM), jnp.float32) * in_scale).astype(jnp.bfloat16)
    w_out = (jax.random.normal(key_o, (NUM_HEADS, HEAD_DIM, MODEL_DIM), jnp.float32) * out_scale).astype(jnp.bfloat16)
    gain_pre = 0.5 * jax.random.normal(key_gp, (MODEL_DIM,), jnp.float32)
    gain_post = 0.5 * jax.random.normal(key_gq, (MODEL_DIM,), jnp.float32)
    return {'x_in': x_in, 'positions': positions, 'grad_out': grad_out, 'w_query': w_query, 'w_key': w_key, 'w_value': w_value, 'w_out': w_out, 'gain_pre': gain_pre, 'gain_post': gain_post}


def rms_norm(hidden, scale_w):
    values = hidden.astype(jnp.float32)
    inv_rms = lax.rsqrt(jnp.mean(values * values, axis=-1, keepdims=True) + NORM_EPS)
    return (values * inv_rms * (1.0 + scale_w)).astype(jnp.bfloat16)


def rope_tables(positions, head_dim):
    half_dim = head_dim // 2
    inv_freq = ROPE_THETA ** (-2.0 * jnp.arange(half_dim, dtype=jnp.float32) / head_dim)
    angles = positions.astype(jnp.float32)[:, :, None] * inv_freq
    return jnp.cos(angles)[:, :, None, :], jnp.sin(angles)[:, :, None, :]


def apply_rope(values, cos_t, sin_t):
    half_dim = values.shape[-1] // 2
    lo_half = values[..., :half_dim]
    hi_half = values[..., half_dim:]
    return jnp.concatenate([lo_half * cos_t - hi_half * sin_t, hi_half * cos_t + lo_half * sin_t], axis=-1)


def block_probs(q_blk, k_blk, pos_q, pos_k):
    scores = jnp.einsum('bqkgd,bskd->bkgqs', q_blk.astype(jnp.float32), k_blk.astype(jnp.float32))
    capped = SOFT_CAP * jnp.tanh(scores / SOFT_CAP)
    pos_gap = pos_q[:, :, None] - pos_k[:, None, :]
    in_window = ((pos_gap >= 0) & (pos_gap < WINDOW))[:, None, None, :, :]
    return jax.nn.softmax(jnp.where(in_window, capped, -1e30), axis=-1)


def attention(q_all, k_all, v_all, positions):
    seq_len = positions.shape[1]
    q_block = min(QUERY_BLOCK, seq_len)
    slab_len = min(WINDOW + q_block, seq_len)

    def one_block(blk_idx):
        q_start = blk_idx * q_block
        k_start = jnp.maximum(q_start + q_block - slab_len, 0)
        q_blk = lax.dynamic_slice_in_dim(q_all, q_start, q_block, axis=1)
        k_blk = lax.dynamic_slice_in_dim(k_all, k_start, slab_len, axis=1)
        v_blk = lax.dynamic_slice_in_dim(v_all, k_start, slab_len, axis=1)
        pos_q = lax.dynamic_slice_in_dim(positions, q_start, q_block, axis=1)
        pos_k = lax.dynamic_slice_in_dim(positions, k_start, slab_len, axis=1)
        prob_blk = block_probs(q_blk, k_blk, pos_q, pos_k)
        out_blk = jnp.einsum('bkgqs,bskd->bqkgd', prob_blk.astype(jnp.bfloat16).astype(jnp.float32), v_blk.astype(jnp.float32))
        return out_blk.astype(jnp.bfloat16)

    blocks = lax.map(jax.checkpoint(one_block), jnp.arange(seq_len // q_block))
    return jnp.moveaxis(blocks, 0, 1).reshape(q_all.shape)


def forward(positions, x_in, w_query, w_key, w_value, w_out, gain_pre, gain_post):
    n_rows, seq_len = positions.shape
    num_heads, head_dim = w_query.shape[1], w_query.shape[2]
    kv_heads = w_key.shape[1]
    normed = rms_norm(x_in, gain_pre).astype(jnp.float32)
    cos_t, sin_t = rope_tables(positions, head_dim)
    q_lin = jnp.einsum('bsd,dhe->bshe', normed, w_query.astype(jnp.float32))
    k_lin = jnp.einsum('bsd,dhe->bshe', normed, w_key.astype(jnp.float32))
    v_lin = jnp.einsum('bsd,dhe->bshe', normed, w_value.astype(jnp.float32))
    q_all = (apply_rope(q_lin, cos_t, sin_t) * head_dim ** -0.5).astype(jnp.bfloat16)
    q_all = q_all.reshape(n_rows, seq_len, kv_heads, num_heads // kv_heads, head_dim)
    k_all = apply_rope(k_lin, cos_t, sin_t).astype(jnp.bfloat16)
    v_all = v_lin.astype(jnp.bfloat16)
    attn_out = attention(q_all, k_all, v_all, positions).reshape(n_rows, seq_len, num_heads, head_dim)
    proj_out = jnp.einsum('bshe,hed->bsd', attn_out.astype(jnp.float32), w_out.astype(jnp.float32)).astype(jnp.bfloat16)
    post_norm = rms_norm(proj_out, gain_post)
    return (x_in.astype(jnp.float32) + post_norm.astype(jnp.float32)).astype(jnp.bfloat16)


def reference(x_in, positions, grad_out, w_query, w_key, w_value, w_out, gain_pre, gain_post):
    y_out, pullback = jax.vjp(functools.partial(forward, positions), x_in, w_query, w_key, w_value, w_out, gain_pre, gain_post)
    grad_x, grad_wq, grad_wk, grad_wv, grad_wo, grad_pre, grad_post = pullback(grad_out)
    return (y_out, grad_x, grad_wq.astype(jnp.float32), grad_wk.astype(jnp.float32), grad_wv.astype(jnp.float32), grad_wo.astype(jnp.float32), grad_pre.astype(jnp.float32), grad_post.astype(jnp.float32))
```

```python
import functools

import jax
import jax.numpy as jnp
from jax import lax
from jax.experimental import pallas as pl
from jax.experimental.pallas import tpu as pltpu
from jax.sharding import PartitionSpec as P

WINDOW = 4096
SOFT_CAP = 50.0
NORM_EPS = 1e-6
ROPE_THETA = 10000.0
BLK = 256
HD = 128
CAP2 = SOFT_CAP * 1.4426950408889634


def rope_tables(positions):
    half = HD // 2
    inv_freq = ROPE_THETA ** (-2.0 * jnp.arange(half, dtype=jnp.float32) / HD)
    angles = positions.astype(jnp.float32)[:, :, None] * inv_freq
    cos, sin = jnp.cos(angles), jnp.sin(angles)
    return jnp.concatenate([cos, cos], -1), jnp.concatenate([-sin, sin], -1)


def block_tables(pos):
    rows, seq = pos.shape
    nb = seq // BLK
    blocks = pos.reshape(rows, nb, BLK)
    first, last = blocks[:, :, 0], blocks[:, :, -1]
    idx = jnp.arange(nb, dtype=jnp.int32)
    meets = (first[:, :, None] - last[:, None, :]) < WINDOW
    whole = (last[:, :, None] - first[:, None, :]) < WINDOW
    q_lo = jnp.sum(~meets, axis=2, dtype=jnp.int32)
    q_full = jnp.minimum(jnp.sum(~whole, axis=2, dtype=jnp.int32), idx)
    k_hi = jnp.sum(meets, axis=1, dtype=jnp.int32)
    k_full = jnp.maximum(jnp.sum(whole, axis=1, dtype=jnp.int32), idx + 1)
    return jnp.stack([q_lo, q_full], 1), jnp.stack([k_full, k_hi], 1)


NT = (((1,), (1,)), ((), ()))
TN = (((0,), (0,)), ((), ()))


def stack_heads(block):
    return jnp.concatenate([block[:, :HD], block[:, HD:]], axis=0)


def rope(x, cos, sin):
    return x * cos + pltpu.roll(x, HD // 2, 1) * sin


def rope_t(x, cos, sin):
    return x * cos - pltpu.roll(x, HD // 2, 1) * sin


def qkv_kernel(a_ref, w_ref, cos_ref, sin_ref, out_ref):
    cos, sin = cos_ref[...], sin_ref[...]
    for g in range(2):
        acc = jnp.dot(a_ref[...], w_ref[:, g * 512:(g + 1) * 512], preferred_element_type=jnp.float32)
        c0 = g * 512
        for h in range(2):
            q = rope(acc[:, h * HD:(h + 1) * HD], cos, sin) * (HD ** -0.5)
            out_ref[:, c0 + h * HD:c0 + (h + 1) * HD] = q.astype(jnp.bfloat16)
        out_ref[:, c0 + 256:c0 + 384] = rope(acc[:, 256:384], cos, sin).astype(jnp.bfloat16)
        out_ref[:, c0 + 384:c0 + 512] = acc[:, 384:512].astype(jnp.bfloat16)


def qkv_project(a, w, cos, sin):
    seq, dim = a.shape
    bm = 512
    return pl.pallas_call(
        qkv_kernel,
        grid=(seq // bm,),
        in_specs=[
            pl.BlockSpec((bm, dim), lambda m: (m, 0)),
            pl.BlockSpec((dim, 1024), lambda m: (0, 0)),
            pl.BlockSpec((bm, HD), lambda m: (m, 0)),
            pl.BlockSpec((bm, HD), lambda m: (m, 0)),
        ],
        out_specs=pl.BlockSpec((bm, 1024), lambda m: (m, 0)),
        out_shape=jax.ShapeDtypeStruct((seq, 1024), jnp.bfloat16),
        cost_estimate=pl.CostEstimate(flops=2 * seq * dim * 1024, bytes_accessed=2 * (seq * dim + dim * 1024 + seq * 1024), transcendentals=0),
        compiler_params=pltpu.CompilerParams(dimension_semantics=("arbitrary",), vmem_limit_bytes=60 * 1024 * 1024),
        name="qkv",
    )(a, w, cos, sin)


def fwd_kernel(tab_ref, q_ref, k_ref, v_ref, posc_ref, posr_ref, o_ref, lse_ref, acc_ref, sum_ref):
    i = pl.program_id(1)
    q = stack_heads(q_ref[...])
    acc_ref[...] = jnp.zeros_like(acc_ref)
    sum_ref[...] = jnp.zeros_like(sum_ref)

    def step(j, masked):
        r0 = pl.multiple_of(j * BLK, BLK)
        k = k_ref[pl.ds(r0, BLK), :]
        v = v_ref[pl.ds(r0, BLK), :]
        s = lax.dot_general(q, k, NT, preferred_element_type=jnp.float32)
        e = jnp.exp2(jnp.tanh(s * (1.0 / SOFT_CAP)) * CAP2)
        if masked:
            gap = posc_ref[...] - posr_ref[:, pl.ds(r0, BLK)]
            keep = (gap >= 0) & (gap < WINDOW)
            keep = jnp.concatenate([keep, keep], axis=0)
            e = jnp.where(keep, e, 0.0)
        sum_ref[...] += e[:, :HD] + e[:, HD:]
        acc_ref[...] += jnp.dot(e.astype(jnp.bfloat16), v, preferred_element_type=jnp.float32)

    lo, full = tab_ref[0, i], tab_ref[1, i]

    @pl.loop(lo, full)
    def _(j):
        step(j, True)

    @pl.loop(jnp.maximum(lo, full), i)
    def _(j):
        step(j, False)

    step(i, True)
    part = sum_ref[...]
    total = jnp.sum(part, axis=1, keepdims=True)
    o = (acc_ref[...] / total).astype(jnp.bfloat16)
    o_ref[:, :HD] = o[:BLK]
    o_ref[:, HD:] = o[BLK:]
    lse_ref[0, pl.ds(i, 1), :] = jnp.log2(jnp.sum(part.T, axis=0, keepdims=True))


def attention_fwd(qkv, tab, pos_col, pos_row):
    seq = qkv.shape[0]
    nb = seq // BLK
    grid_spec = pltpu.PrefetchScalarGridSpec(
        num_scalar_prefetch=1,
        grid=(2, nb),
        in_specs=[
            pl.BlockSpec((BLK, 256), lambda g, i, t: (i, 2 * g)),
            pl.BlockSpec((seq, HD), lambda g, i, t: (0, 4 * g + 2)),
            pl.BlockSpec((seq, HD), lambda g, i, t: (0, 4 * g + 3)),
            pl.BlockSpec((BLK, 1), lambda g, i, t: (i, 0)),
            pl.BlockSpec((1, seq), lambda g, i, t: (0, 0)),
        ],
        out_specs=[
            pl.BlockSpec((BLK, 256), lambda g, i, t: (i, g)),
            pl.BlockSpec((1, nb, 2 * BLK), lambda g, i, t: (g, 0, 0)),
        ],
        scratch_shapes=[pltpu.VMEM((2 * BLK, HD), jnp.float32), pltpu.VMEM((2 * BLK, HD), jnp.float32)],
    )
    return pl.pallas_call(
        fwd_kernel,
        grid_spec=grid_spec,
        out_shape=[jax.ShapeDtypeStruct((seq, 512), jnp.bfloat16), jax.ShapeDtypeStruct((2, nb, 2 * BLK), jnp.float32)],
        cost_estimate=pl.CostEstimate(flops=4 * seq * seq * 512, bytes_accessed=4 * seq * 1024, transcendentals=seq * seq * 4),
        compiler_params=pltpu.CompilerParams(dimension_semantics=("arbitrary", "arbitrary"), vmem_limit_bytes=48 * 1024 * 1024),
        name="attn_fwd",
    )(tab, qkv, qkv, qkv, pos_col, pos_row)


def bwd_kernel(tab_ref, q_ref, k_ref, v_ref, o_ref, do_ref, lse_ref, posc_ref, posr_ref, cos_ref, sin_ref,
               out_ref, dq_ref, dk_ref, dv_ref, delta_ref):
    j = pl.program_id(1)
    nb = pl.num_programs(1)

    @pl.when(j == 0)
    def _():
        dq_ref[...] = jnp.zeros_like(dq_ref)

        @pl.loop(0, nb)
        def _(i):
            r0 = pl.multiple_of(i * BLK, BLK)
            prod = o_ref[pl.ds(r0, BLK), :].astype(jnp.float32) * do_ref[pl.ds(r0, BLK), :].astype(jnp.float32)
            delta_ref[pl.ds(i, 1), :] = jnp.sum(stack_heads(prod).T, axis=0, keepdims=True)

    k = k_ref[...]
    v = v_ref[...]
    dk_ref[...] = jnp.zeros_like(dk_ref)
    dv_ref[...] = jnp.zeros_like(dv_ref)

    def step(i, masked):
        r0 = pl.multiple_of(i * BLK, BLK)
        q = stack_heads(q_ref[pl.ds(r0, BLK), :])
        do = stack_heads(do_ref[pl.ds(r0, BLK), :])
        s = lax.dot_general(k, q, NT, preferred_element_type=jnp.float32)
        dp = lax.dot_general(v, do, NT, preferred_element_type=jnp.float32)
        t = jnp.tanh(s * (1.0 / SOFT_CAP))
        p = jnp.exp2(t * CAP2 - lse_ref[0, pl.ds(i, 1), :])
        if masked:
            gap = posr_ref[:, pl.ds(r0, BLK)] - posc_ref[...]
            keep = (gap >= 0) & (gap < WINDOW)
            keep = jnp.concatenate([keep, keep], axis=1)
            p = jnp.where(keep, p, 0.0)
        ds = p * (dp - delta_ref[pl.ds(i, 1), :]) * (1.0 - t * t)
        pb = p.astype(jnp.bfloat16)
        dsb = ds.astype(jnp.bfloat16)
        dv_ref[...] += jnp.dot(pb, do, preferred_element_type=jnp.float32)
        dk_ref[...] += jnp.dot(dsb, q, preferred_element_type=jnp.float32)
        dq = lax.dot_general(dsb, k, TN, preferred_element_type=jnp.float32)
        dq_ref[pl.ds(r0, BLK), :HD] += dq[:BLK]
        dq_ref[pl.ds(r0, BLK), HD:] += dq[BLK:]

    full, hi = tab_ref[0, j], tab_ref[1, j]
    step(j, True)

    @pl.loop(j + 1, jnp.minimum(full, hi))
    def _(i):
        step(i, False)

    @pl.loop(full, hi)
    def _(i):
        step(i, True)

    r0 = pl.multiple_of(j * BLK, BLK)
    cos, sin = cos_ref[pl.ds(r0, BLK), :], sin_ref[pl.ds(r0, BLK), :]
    out_ref[pl.ds(r0, BLK), 256:384] = rope_t(dk_ref[...], cos, sin).astype(jnp.bfloat16)
    out_ref[pl.ds(r0, BLK), 384:512] = dv_ref[...].astype(jnp.bfloat16)

    @pl.when(j == nb - 1)
    def _():
        @pl.loop(0, nb)
        def _(i):
            s0 = pl.multiple_of(i * BLK, BLK)
            c, s = cos_ref[pl.ds(s0, BLK), :], sin_ref[pl.ds(s0, BLK), :]
            for h in range(2):
                dq = rope_t(dq_ref[pl.ds(s0, BLK), h * HD:(h + 1) * HD], c, s) * (HD ** -0.5)
                out_ref[pl.ds(s0, BLK), h * HD:(h + 1) * HD] = dq.astype(jnp.bfloat16)


def attention_bwd(qkv, o, do, lse, tab, pos_col, pos_row, cos, sin):
    seq = qkv.shape[0]
    nb = seq // BLK
    grid_spec = pltpu.PrefetchScalarGridSpec(
        num_scalar_prefetch=1,
        grid=(2, nb),
        in_specs=[
            pl.BlockSpec((seq, 256), lambda g, j, t: (0, 2 * g)),
            pl.BlockSpec((BLK, HD), lambda g, j, t: (j, 4 * g + 2)),
            pl.BlockSpec((BLK, HD), lambda g, j, t: (j, 4 * g + 3)),
            pl.BlockSpec((seq, 256), lambda g, j, t: (0, g)),
            pl.BlockSpec((seq, 256), lambda g, j, t: (0, g)),
            pl.BlockSpec((1, nb, 2 * BLK), lambda g, j, t: (g, 0, 0)),
            pl.BlockSpec((BLK, 1), lambda g, j, t: (j, 0)),
            pl.BlockSpec((1, seq), lambda g, j, t: (0, 0)),
            pl.BlockSpec((seq, HD), lambda g, j, t: (0, 0)),
            pl.BlockSpec((seq, HD), lambda g, j, t: (0, 0)),
        ],
        out_specs=pl.BlockSpec((seq, 512), lambda g, j, t: (0, g)),
        scratch_shapes=[
            pltpu.VMEM((seq, 256), jnp.float32),
            pltpu.VMEM((BLK, HD), jnp.float32),
            pltpu.VMEM((BLK, HD), jnp.float32),
            pltpu.VMEM((nb, 2 * BLK), jnp.float32),
        ],
    )
    return pl.pallas_call(
        bwd_kernel,
        grid_spec=grid_spec,
        out_shape=jax.ShapeDtypeStruct((seq, 1024), jnp.bfloat16),
        cost_estimate=pl.CostEstimate(flops=10 * seq * seq * 512, bytes_accessed=6 * seq * 1024, transcendentals=seq * seq * 4),
        compiler_params=pltpu.CompilerParams(dimension_semantics=("arbitrary", "arbitrary"), vmem_limit_bytes=48 * 1024 * 1024),
        name="attn_bwd",
    )(tab, qkv, qkv, qkv, o, do, lse, pos_col, pos_row, cos, sin)


ROW_BLK = 128


def pre_kernel(x_ref, gain_ref, out_ref):
    x = x_ref[0].astype(jnp.float32)
    inv = lax.rsqrt(jnp.mean(x * x, axis=-1, keepdims=True) + NORM_EPS)
    out_ref[...] = (x * inv * (1.0 + gain_ref[...])).astype(jnp.bfloat16)


def pre_norm(x_in, gain, b):
    _, tok, dim = x_in.shape
    return pl.pallas_call(
        pre_kernel,
        grid=(tok // ROW_BLK,),
        in_specs=[
            pl.BlockSpec((1, ROW_BLK, dim), lambda m: (b, m, 0)),
            pl.BlockSpec((1, dim), lambda m: (0, 0)),
        ],
        out_specs=pl.BlockSpec((ROW_BLK, dim), lambda m: (m, 0)),
        out_shape=jax.ShapeDtypeStruct((tok, dim), jnp.bfloat16),
        cost_estimate=pl.CostEstimate(flops=8 * tok * dim, bytes_accessed=4 * tok * dim, transcendentals=tok),
        name="pre_norm",
    )(x_in, gain)


def fold_rows(x):
    return jnp.sum(x.reshape(x.shape[0] // 8, 8, x.shape[1]), axis=0)


def rms_bwd(u, g, gain):
    inv = lax.rsqrt(jnp.mean(u * u, axis=-1, keepdims=True) + NORM_EPS)
    normed = u * inv
    d_gain = fold_rows(g * normed)
    h = g * (1.0 + gain)
    d_u = inv * (h - normed * jnp.mean(h * normed, axis=-1, keepdims=True))
    return d_u, d_gain


def post_kernel(n_parts, has_prev, *refs):
    parts, (x_ref, g_ref, gain_ref) = refs[:n_parts], refs[n_parts:n_parts + 3]
    y_ref, dr_ref, dgain_ref = refs[-3:]
    r = parts[0][...].astype(jnp.float32)
    for p in parts[1:]:
        r = (r + p[...].astype(jnp.float32))
    r = r.astype(jnp.bfloat16).astype(jnp.float32)
    gain = gain_ref[...]
    g = g_ref[0].astype(jnp.float32)
    inv = lax.rsqrt(jnp.mean(r * r, axis=-1, keepdims=True) + NORM_EPS)
    post = (r * inv * (1.0 + gain)).astype(jnp.bfloat16)
    y_ref[0] = (x_ref[0].astype(jnp.float32) + post.astype(jnp.float32)).astype(jnp.bfloat16)
    d_r, d_gain = rms_bwd(r, g, gain)
    dr_ref[...] = d_r.astype(jnp.bfloat16)

    @pl.when(pl.program_id(0) == 0)
    def _():
        dgain_ref[...] = jnp.zeros_like(dgain_ref)

    dgain_ref[...] += d_gain


def final_kernel(n_parts, has_prev, *refs):
    parts, (x_ref, g_ref, gain_ref) = refs[:n_parts], refs[n_parts:n_parts + 3]
    gx_ref, dgain_ref = refs[-2:]
    da = parts[0][...].astype(jnp.float32)
    for p in parts[1:]:
        da = (da + p[...].astype(jnp.float32))
    da = da.astype(jnp.bfloat16).astype(jnp.float32)
    d_x, d_gain = rms_bwd(x_ref[0].astype(jnp.float32), da, gain_ref[...])
    d_x = d_x.astype(jnp.bfloat16).astype(jnp.float32)
    gx_ref[0] = (g_ref[0].astype(jnp.float32) + d_x).astype(jnp.bfloat16)

    @pl.when(pl.program_id(0) == 0)
    def _():
        dgain_ref[...] = jnp.zeros_like(dgain_ref)

    dgain_ref[...] += d_gain


def token_stage(kernel, name, parts, x_in, grad_out, gain, b, prev, with_dr):
    n_rows, tok, dim = x_in.shape
    blk = pl.BlockSpec((ROW_BLK, dim), lambda m: (m, 0))
    row = pl.BlockSpec((1, ROW_BLK, dim), lambda m: (b, m, 0))
    args = [*parts, x_in, grad_out, gain]
    in_specs = [blk] * len(parts) + [row, row, pl.BlockSpec((1, dim), lambda m: (0, 0))]
    alias = {}
    if prev is not None:
        alias = {len(args): 0}
        args.append(prev)
        in_specs.append(pl.BlockSpec(memory_space=pl.ANY))
    out_shape = [jax.ShapeDtypeStruct(x_in.shape, jnp.bfloat16)]
    out_specs = [row]
    if with_dr:
        out_shape.append(jax.ShapeDtypeStruct((tok, dim), jnp.bfloat16))
        out_specs.append(blk)
    out_shape.append(jax.ShapeDtypeStruct((8, dim), jnp.float32))
    out_specs.append(pl.BlockSpec((8, dim), lambda m: (0, 0)))
    return pl.pallas_call(
        functools.partial(kernel, len(parts), prev is not None),
        grid=(tok // ROW_BLK,),
        in_specs=in_specs,
        out_specs=out_specs,
        out_shape=out_shape,
        input_output_aliases=alias,
        cost_estimate=pl.CostEstimate(flops=30 * tok * dim, bytes_accessed=10 * tok * dim, transcendentals=tok),
        compiler_params=pltpu.CompilerParams(dimension_semantics=("arbitrary",), vmem_limit_bytes=40 * 1024 * 1024),
        name=name,
    )(*args)


def solution(mesh):
    act_spec = P('dp', 'tp', None)
    head_spec = P(None, 'tp', None)
    grad_spec = P('dp', 'tp', None)
    in_specs = (act_spec, P('dp', 'tp'), act_spec, head_spec, head_spec, head_spec, P('tp', None, None), P(None), P(None))
    out_specs = (act_spec, act_spec, grad_spec, grad_spec, grad_spec, P(('dp', 'tp'), None, None), P('dp'), P('dp'))
    f32 = jnp.float32

    def local_step(x_in, positions, grad_out, w_query, w_key, w_value, w_out, gain_pre, gain_post):
        n_rows, dim = x_in.shape[0], x_in.shape[2]
        rows = range(n_rows)
        w_o = w_out.reshape(512, dim)
        w_qkv = jnp.concatenate(
            [w_query[:, 0], w_query[:, 1], w_key[:, 0], w_value[:, 0], w_query[:, 2], w_query[:, 3], w_key[:, 1], w_value[:, 1]], axis=1)

        gain_pre2, gain_post2 = gain_pre[None, :], gain_post[None, :]
        normed = [lax.all_gather(pre_norm(x_in, gain_pre2, b), 'tp', axis=0, tiled=True) for b in rows]
        pos = lax.all_gather(positions, 'tp', axis=1, tiled=True)
        cos, sin = rope_tables(pos)
        q_tab, k_tab = block_tables(pos)

        qkv, o, lse, dqkv, dr = {}, {}, {}, {}, {}
        y_out, grad_x = None, None
        g_post, g_pre = [], []
        g_wo = None
        for b in rows:
            pos_col, pos_row = pos[b][:, None], pos[b][None, :]
            qkv[b] = qkv_project(normed[b], w_qkv, cos[b], sin[b])
            o[b], lse[b] = attention_fwd(qkv[b], q_tab[b], pos_col, pos_row)
            part = jnp.dot(o[b], w_o, preferred_element_type=f32).astype(jnp.bfloat16)
            proj = lax.psum_scatter(part, 'tp', scatter_dimension=0, tiled=True)
            y_out, d_proj, d_gain = token_stage(post_kernel, "post_norm", [proj], x_in, grad_out, gain_post2, b, y_out, True)
            g_post.append(d_gain)
            dr[b] = lax.all_gather(d_proj, 'tp', axis=0, tiled=True)
        for b in rows:
            pos_col, pos_row = pos[b][:, None], pos[b][None, :]
            d_attn = lax.dot_general(dr[b], w_o, NT, preferred_element_type=f32).astype(jnp.bfloat16)
            dqkv[b] = attention_bwd(qkv[b], o[b], d_attn, lse[b], k_tab[b], pos_col, pos_row, cos[b], sin[b])
            d_a = lax.dot_general(dqkv[b], w_qkv, NT, preferred_element_type=f32).astype(jnp.bfloat16)
            d_a_loc = lax.psum_scatter(d_a, 'tp', scatter_dimension=0, tiled=True)
            grad_x, d_gain = token_stage(final_kernel, "pre_norm_bwd", [d_a_loc], x_in, grad_out, gain_pre2, b, grad_x, False)
            g_pre.append(d_gain)
        g_w = None
        for b in rows:
            t = lax.dot_general(o[b], dr[b], TN, preferred_element_type=f32)
            g_wo = t if g_wo is None else g_wo + t
            t = lax.dot_general(normed[b], dqkv[b], TN, preferred_element_type=f32)
            g_w = t if g_w is None else g_w + t
        grad_wq = jnp.stack([g_w[:, 0:128], g_w[:, 128:256], g_w[:, 512:640], g_w[:, 640:768]], axis=1)
        grad_wk = jnp.stack([g_w[:, 256:384], g_w[:, 768:896]], axis=1)
        grad_wv = jnp.stack([g_w[:, 384:512], g_w[:, 896:1024]], axis=1)
        grad_wo = g_wo.reshape(4, 128, dim)
        grad_pre = lax.psum(jnp.sum(sum(g_pre), axis=0), 'tp')
        grad_post = lax.psum(jnp.sum(sum(g_post), axis=0), 'tp')
        return y_out, grad_x, grad_wq, grad_wk, grad_wv, grad_wo, grad_pre, grad_post

    return jax.shard_map(local_step, mesh=mesh, in_specs=in_specs, out_specs=out_specs, check_vma=False)
```
